32 devices in a mesh: batch: 4 (over y, x), ctx: 8 (over z, core).
Axes of the slice: x: 2, y: 2, z: 4, core: 2. Of those that a mesh axis runs over, the one named last changes fastest.
Arguments:
- asked_for: bfloat16 [4, 1024, 64, 64], P('batch', 'ctx'), may hold values from -6 to 6
- offered: bfloat16 [4, 1024, 64, 64], P('batch', 'ctx'), may hold values from -6 to 6
- contents: bfloat16 [4, 1024, 64, 64], P('batch', 'ctx'), may hold values from -6 to 6
- out_weight: bfloat16 [4096, 4096], P('batch'), may hold values from -0.09375 to 0.09375
Outputs:
- layer_out: bfloat16 [4, 1024, 4096], P('batch', 'ctx')
The draws below stay inside these ranges and needn't reach their ends.
All inputs are finite; a program needn't handle non-finite values.
Results may differ from the reference program's by a relative error of at most 0.006.
Values may be sent and summed in bfloat16 or wider, within the bound.
No kernel may reach another device: no remote copies, remote signals or barrier semaphores. Data moves between devices by JAX's collectives and lax.ppermute only.
A program may use at most 128 MiB of HBM per device.

```python
import jax
import jax.numpy as jnp
from jax import lax

HEADS = 64
HEAD_SIZE = 64
BATCH = 4
TOKENS = 1024
WIDTH = 4096


def shard_levels(key, dims, split, least, top_value):
    level = 1.0
    for axis_at, shards_of in split:
        steps = jax.random.uniform(jax.random.fold_in(jax.random.fold_in(key, 6), axis_at), (shards_of,), jnp.float32, least / len(split), top_value / len(split))
        level = level * jnp.repeat(jnp.exp(steps), dims[axis_at] // shards_of).reshape((-1,) + (1,) * (len(dims) - 1 - axis_at))
    return level


def centred(rng, extent, width, bound, pieces=(), kind=jnp.bfloat16):
    entries = jax.random.normal(rng, extent, jnp.float32) * width
    if len(pieces) > 0:
        entries = shard_levels(rng, extent, pieces, -0.22, 0.18) * entries
    return jnp.clip(entries, min=-bound, max=bound).astype(kind)


def setup_inputs(seed: int = 0) -> dict:
    key_of = jax.random.split(jax.random.key(seed), 5)
    return {
        "asked_for": centred(key_of[0], (BATCH, TOKENS, HEADS, HEAD_SIZE), 1.0, 6.0, ((0, 4), (1, 8))),
        "offered": centred(key_of[1], (BATCH, TOKENS, HEADS, HEAD_SIZE), 1.0, 6.0, ((0, 4), (1, 8))),
        "contents": centred(key_of[2], (BATCH, TOKENS, HEADS, HEAD_SIZE), 1.0, 6.0, ((0, 4), (1, 8))),
        "out_weight": centred(key_of[3], (WIDTH, WIDTH), WIDTH ** -0.5, 0.09375, ((0, 4),)),
    }


def to_features(values):
    wide = values.astype(jnp.float32)
    return (jax.nn.softplus(wide)).astype(jnp.bfloat16)


def after_reading(read, count):
    result = read * count ** 0.5
    return result.astype(jnp.bfloat16)


def look_up(features, state, mass):
    small = lax.optimization_barrier(state.astype(jnp.bfloat16))
    top = jnp.einsum("bthd,bhde->bthe", features.astype(jnp.float32), small.astype(jnp.float32))
    bottom = jnp.einsum("bthd,bhd->bth", features.astype(jnp.float32), mass, precision=lax.Precision.HIGHEST)
    return top / (bottom + 1e-3)[..., None]


def reference(asked_for, offered, contents, out_weight):
    query_feature, key_feature = lax.optimization_barrier((to_features(asked_for), to_features(offered)))
    state = jnp.einsum("bthd,bthe->bhde", key_feature.astype(jnp.float32), contents.astype(jnp.float32)) / TOKENS
    mass = jnp.sum(key_feature.astype(jnp.float32), axis=1) / TOKENS
    mixed = after_reading(look_up(query_feature, state, mass), TOKENS).reshape(BATCH, TOKENS, WIDTH)
    mixed = lax.optimization_barrier(mixed)
    layer_out = jnp.einsum("btw,wv->btv", mixed.astype(jnp.float32), out_weight.astype(jnp.float32)).astype(jnp.bfloat16)
    return layer_out
```

```python
import jax
import jax.numpy as jnp
from jax import lax
from jax.sharding import PartitionSpec as P


def to_features(values):
    wide = values.astype(jnp.float32)
    return jax.nn.softplus(wide).astype(jnp.bfloat16)


def partner(step, size):
    if size & (size - 1) == 0:
        return [(i, i ^ step) for i in range(size)]
    return [(i, (i + step) % size) for i in range(size)]


def target(me, step, size):
    return me ^ step if size & (size - 1) == 0 else (me + step) % size


def origin(me, step, size):
    return me ^ step if size & (size - 1) == 0 else (me - step) % size


def shards(asked_for, offered, contents, out_weight):
    nb, nc = lax.axis_size("batch"), lax.axis_size("ctx")
    _, tokens, heads, size = asked_for.shape
    count = tokens * nc
    width = heads * size
    part = width // nb
    me = lax.axis_index("batch")

    query = asked_for.reshape(tokens, nb, part).transpose(1, 0, 2)
    query = lax.all_to_all(query, "batch", split_axis=0, concat_axis=0, tiled=True)
    query = to_features(query)

    key = to_features(offered).reshape(tokens, heads, size)
    value = contents.reshape(tokens, heads, size)
    state = jnp.einsum("thd,the->dhe", key, value, preferred_element_type=jnp.float32)
    state = state.reshape(size, width)
    mass = jnp.sum(key.astype(jnp.float32), axis=0).reshape(1, width)
    packed = jnp.concatenate([state, jnp.broadcast_to(mass, (16, width))], axis=0) / count
    packed = packed.astype(jnp.bfloat16)
    piece = width // (nb * nc)
    rows = size + 16
    packed = packed.reshape(rows, nb, nc, piece).transpose(1, 2, 0, 3).reshape(nb * nc, rows, piece)
    packed = lax.all_to_all(packed, ("batch", "ctx"), split_axis=0, concat_axis=0, tiled=True)
    total = jnp.sum(packed.reshape(nb, nc, rows, piece).astype(jnp.float32), axis=1)
    total = total.astype(jnp.bfloat16)
    total = lax.all_gather(total, "ctx", axis=0)
    total = total.transpose(1, 2, 0, 3).reshape(nb, rows, part)
    own = part // size
    state = total[:, :size].reshape(nb, size, own, size)
    mass = total[:, size].reshape(nb, own, size).astype(jnp.float32)

    split = query.reshape(nb, tokens, own, size)
    top = jnp.einsum("bthd,bdhe->bthe", split, state, preferred_element_type=jnp.float32)
    bottom = jnp.einsum("bthd,bhd->bth", split.astype(jnp.float32), mass)
    mixed = top / (bottom + 0.001)[..., None] * count**0.5
    mixed = mixed.astype(jnp.bfloat16).reshape(nb, tokens, part)

    def project(at):
        rows = lax.dynamic_index_in_dim(mixed, at, 0, keepdims=False)
        return jnp.dot(rows, out_weight, preferred_element_type=jnp.float32)

    arrived = []
    for step in range(nb - 1, 0, -1):
        sent = project(target(me, step, nb)).astype(jnp.bfloat16)
        arrived.append(lax.ppermute(sent, "batch", partner(step, nb)))
    out = project(me)
    for other in arrived:
        out = out + other.astype(jnp.float32)
    return out.astype(jnp.bfloat16)[None]


def solution(mesh):
    in_specs = (
        P("batch", "ctx", None, None),
        P("batch", "ctx", None, None),
        P("batch", "ctx", None, None),
        P("batch", None),
    )
    out_specs = P("batch", "ctx", None)
    return jax.shard_map(shards, mesh=mesh, in_specs=in_specs, out_specs=out_specs, check_vma=False)
```

```python
import jax
import jax.numpy as jnp
from jax import lax
from jax.sharding import PartitionSpec as P

F32, BF16 = jnp.float32, jnp.bfloat16


def to_features(values):
    return jax.nn.softplus(values.astype(F32)).astype(BF16)


def grid_of(size):
    inner = 1
    while inner * inner * 4 <= size and size % (inner * 2) == 0:
        inner *= 2
    if inner * inner < size and size % (inner * 2) == 0 and inner * 2 * inner * 2 <= size * 2:
        inner *= 2
    return size // inner, inner


def moves(ny, nx, dy, dx):
    return [(y * nx + x, (y + dy) % ny * nx + (x + dx) % nx) for y in range(ny) for x in range(nx)]


def rows_times(left, right):
    return lax.dot_general(left, right, (((0,), (0,)), ((), ())), preferred_element_type=F32)


def shards(asked_for, offered, contents, out_weight):
    nb, nc = lax.axis_size("batch"), lax.axis_size("ctx")
    ny, nx = grid_of(nb)
    _, tokens, heads, size = asked_for.shape
    count = tokens * nc
    width = heads * size
    part, columns = out_weight.shape
    half = columns // 2
    me, at = lax.axis_index("batch"), lax.axis_index("ctx")
    my, mx = me // nx, me % nx
    cores = 2 if nc % 2 == 0 else 1
    core = at % cores
    slab = part // cores

    piece = lax.dynamic_slice_in_dim(out_weight, core * slab, slab, 0)
    swap = [(i, i ^ 1) for i in range(nc)]

    def fetched(block, perm):
        near = lax.ppermute(block, "batch", perm)
        if cores == 1:
            return (near,)
        return near, lax.ppermute(near, "ctx", swap)

    fetch_x = [fetched(piece[:, :half], moves(ny, nx, 0, -j)) for j in range(1, nx)]
    fetch_y = [fetched(piece[:, half:], moves(ny, nx, -j, 0)) for j in range(1, ny)]

    pairs, lanes = heads // 2, 2 * size
    paired = lambda v: v[0].transpose(1, 2, 0).reshape(pairs, lanes, tokens)
    key, value = to_features(paired(offered)), paired(contents)
    both = jnp.einsum("pdt,pet->pde", key, value, preferred_element_type=F32)
    low = lax.broadcasted_iota(jnp.int32, (1, 1, lanes), 2) < size
    state = jnp.where(low, both[:, :size], both[:, size:])
    mass = jnp.einsum("rt,pdt->prd", jnp.ones((8, tokens), BF16), key, preferred_element_type=F32)
    packed = (jnp.concatenate([state, mass], axis=1) / count).astype(BF16)
    rows = size + 8
    packed = packed.reshape(nc, pairs // nc, rows, lanes)
    packed = lax.all_to_all(packed, "ctx", split_axis=0, concat_axis=0, tiled=True)
    total = jnp.sum(packed.astype(F32), axis=0).astype(BF16)
    total = lax.all_gather(total, "ctx", axis=0, tiled=True)
    state, mass = total[:, :size], total[:, size : size + 1]

    query = to_features(paired(asked_for))
    zero = jnp.zeros((), BF16)
    upper = lax.broadcasted_iota(jnp.int32, (1, lanes, 1), 1) < size
    same = low == upper
    wide = jnp.where(same, jnp.concatenate([state, state], axis=1), zero)
    heavy = jnp.where(same, jnp.broadcast_to(mass, (pairs, lanes, lanes)), zero)
    top = jnp.einsum("pde,pdt->pet", wide, query, preferred_element_type=F32)
    bottom = jnp.einsum("ped,pdt->pet", heavy, query, preferred_element_type=F32)
    mixed = (top / (bottom + 0.001) * count**0.5).astype(BF16)
    mixed = mixed.reshape(ny, nx, part, tokens)

    def of_y(y):
        return lax.dynamic_index_in_dim(mixed, y, 0, keepdims=False)

    def of_x(x):
        return lax.dynamic_index_in_dim(mixed, x, 1, keepdims=False)

    def partial(chosen, mine, size_of, weight, fetches):
        pick = lambda i: lax.dynamic_index_in_dim(chosen, i % size_of, 0, keepdims=False)
        out = rows_times(pick(mine), weight)
        for j, pieces in enumerate(fetches, 1):
            block = pick(mine + j)
            for k, got in enumerate(pieces):
                which = core if k == 0 else 1 - core
                out = out + rows_times(lax.dynamic_slice_in_dim(block, which * slab, slab, 0), got)
        return out

    first, second = out_weight[:, :half], out_weight[:, half:]
    came_y = [lax.ppermute(of_y((my + j) % ny), "batch", moves(ny, nx, j, 0)) for j in range(1, ny)]
    came_x = [lax.ppermute(of_x((mx + j) % nx), "batch", moves(ny, nx, 0, j)) for j in range(1, nx)]
    back_y = [
        lax.ppermute(partial(c, mx, nx, first, fetch_x).astype(BF16), "batch", moves(ny, nx, -j, 0))
        for j, c in enumerate(came_y, 1)
    ]
    back_x = [
        lax.ppermute(partial(c, my, ny, second, fetch_y).astype(BF16), "batch", moves(ny, nx, 0, -j))
        for j, c in enumerate(came_x, 1)
    ]
    left = partial(of_y(my), mx, nx, first, fetch_x)
    for got in back_y:
        left = left + got.astype(F32)
    right = partial(of_x(mx), my, ny, second, fetch_y)
    for got in back_x:
        right = right + got.astype(F32)
    return jnp.concatenate([left, right], axis=1).astype(BF16)[None]


def solution(mesh):
    in_specs = (
        P("batch", "ctx", None, None),
        P("batch", "ctx", None, None),
        P("batch", "ctx", None, None),
        P("batch", None),
    )
    out_specs = P("batch", "ctx", None)
    return jax.shard_map(shards, mesh=mesh, in_specs=in_specs, out_specs=out_specs, check_vma=False)
```

```python
import jax
import jax.numpy as jnp
from jax import lax
from jax.sharding import PartitionSpec as P

F32, BF16 = jnp.float32, jnp.bfloat16


def to_features(values):
    return jax.nn.softplus(values.astype(F32)).astype(BF16)


def grid_of(size):
    inner = 1
    while inner * inner * 4 <= size and size % (inner * 2) == 0:
        inner *= 2
    if inner * inner < size and size % (inner * 2) == 0 and inner * 2 * inner * 2 <= size * 2:
        inner *= 2
    return size // inner, inner


def moves(ny, nx, dy, dx):
    return [(y * nx + x, (y + dy) % ny * nx + (x + dx) % nx) for y in range(ny) for x in range(nx)]


def rows_times(left, right):
    return lax.dot_general(left, right, (((0,), (0,)), ((), ())), preferred_element_type=F32)


def shards(asked_for, offered, contents, out_weight):
    nb, nc = lax.axis_size("batch"), lax.axis_size("ctx")
    ny, nx = grid_of(nb)
    _, tokens, heads, size = asked_for.shape
    count = tokens * nc
    part, columns = out_weight.shape
    half = columns // 2
    me, at = lax.axis_index("batch"), lax.axis_index("ctx")
    my, mx = me // nx, me % nx
    cores = 2 if nc % 2 == 0 else 1
    core = at % cores
    slab = part // cores

    def piece(column):
        return lax.dynamic_slice(out_weight, (core * slab, column), (slab, half))

    swap = [(i, i ^ 1) for i in range(nc)]

    def fetched(block, perm):
        near = lax.ppermute(block, "batch", perm)
        if cores == 1:
            return (near,)
        return near, lax.ppermute(near, "ctx", swap)

    fetch_x = [fetched(piece(0), moves(ny, nx, 0, -j)) for j in range(1, nx)]
    fetch_y = [fetched(piece(half), moves(ny, nx, -j, 0)) for j in range(1, ny)]

    pairs, lanes = heads // 2, 2 * size
    paired = lambda v: v[0].transpose(1, 2, 0).reshape(pairs, lanes, tokens)
    key = to_features(paired(offered))
    value = paired(contents)
    both = jnp.einsum("pdt,pet->pde", key, value, preferred_element_type=F32)
    low = lax.broadcasted_iota(jnp.int32, (1, 1, lanes), 2) < size
    state = jnp.where(low, both[:, :size], both[:, size:])
    mass = jnp.einsum("rt,pdt->prd", jnp.ones((8, tokens), BF16), key, preferred_element_type=F32)
    packed = (jnp.concatenate([state, mass], axis=1) / count).astype(BF16)
    rows = size + 8
    packed = packed.reshape(nc, pairs // nc, rows, lanes)
    packed = lax.all_to_all(packed, "ctx", split_axis=0, concat_axis=0, tiled=True)
    total = jnp.sum(packed.astype(F32), axis=0).astype(BF16)
    total = lax.all_gather(total, "ctx", axis=0, tiled=True)
    state, mass = total[:, :size], total[:, size : size + 1]

    query = to_features(paired(asked_for))
    zero = jnp.zeros((), BF16)
    upper = lax.broadcasted_iota(jnp.int32, (1, lanes, 1), 1) < size
    same = low == upper
    wide = jnp.where(same, jnp.concatenate([state, state], axis=1), zero)
    heavy = jnp.where(same, jnp.broadcast_to(mass, (pairs, lanes, lanes)), zero)
    top = jnp.einsum("pde,pdt->pet", wide, query, preferred_element_type=F32)
    bottom = jnp.einsum("ped,pdt->pet", heavy, query, preferred_element_type=F32)
    mixed = (top / (bottom + 0.001) * count**0.5).astype(BF16)
    mixed = mixed.reshape(ny, nx, part, tokens)

    def of_y(y):
        return lax.dynamic_index_in_dim(mixed, y, 0, keepdims=False)

    def of_x(x):
        return lax.dynamic_index_in_dim(mixed, x, 1, keepdims=False)

    def partial(chosen, mine, size_of, weight, fetches):
        pick = lambda i: lax.dynamic_index_in_dim(chosen, i % size_of, 0, keepdims=False)
        out = rows_times(pick(mine), weight)
        for j, pieces in enumerate(fetches, 1):
            block = pick(mine + j)
            for k, got in enumerate(pieces):
                which = core if k == 0 else 1 - core
                out = out + rows_times(lax.dynamic_slice_in_dim(block, which * slab, slab, 0), got)
        return out

    first, second = out_weight[:, :half], out_weight[:, half:]
    came_y = [lax.ppermute(of_y((my + j) % ny), "batch", moves(ny, nx, j, 0)) for j in range(1, ny)]
    came_x = [lax.ppermute(of_x((mx + j) % nx), "batch", moves(ny, nx, 0, j)) for j in range(1, nx)]
    back_y, back_x = [], []
    for j, rows_y in enumerate(came_y, 1):
        sent = partial(rows_y, mx, nx, first, fetch_x).astype(BF16)
        sent, came_x, mixed = lax.optimization_barrier((sent, came_x, mixed))
        back_y.append(lax.ppermute(sent, "batch", moves(ny, nx, -j, 0)))
    for j, rows_x in enumerate(came_x, 1):
        sent = partial(rows_x, my, ny, second, fetch_y).astype(BF16)
        sent, mixed = lax.optimization_barrier((sent, mixed))
        back_x.append(lax.ppermute(sent, "batch", moves(ny, nx, 0, -j)))
    left = partial(of_y(my), mx, nx, first, fetch_x)
    for got in back_y:
        left = left + got.astype(F32)
    right = partial(of_x(mx), my, ny, second, fetch_y)
    for got in back_x:
        right = right + got.astype(F32)
    return jnp.concatenate([left, right], axis=1).astype(BF16)[None]


def solution(mesh):
    in_specs = (
        P("batch", "ctx", None, None),
        P("batch", "ctx", None, None),
        P("batch", "ctx", None, None),
        P("batch", None),
    )
    out_specs = P("batch", "ctx", None)

    return jax.shard_map(shards, mesh=mesh, in_specs=in_specs, out_specs=out_specs, check_vma=False)
```

```python
import jax
import jax.numpy as jnp
from jax import lax
from jax.sharding import PartitionSpec as P

F32, BF16 = jnp.float32, jnp.bfloat16


def to_features(values):
    return jax.nn.softplus(values.astype(F32)).astype(BF16)


def grid_of(size):
    inner = 1
    while inner * inner * 4 <= size and size % (inner * 2) == 0:
        inner *= 2
    if inner * inner < size and size % (inner * 2) == 0 and inner * 2 * inner * 2 <= size * 2:
        inner *= 2
    return size // inner, inner


def moves(ny, nx, dy, dx):
    return [(y * nx + x, (y + dy) % ny * nx + (x + dx) % nx) for y in range(ny) for x in range(nx)]


def rows_times(left, right):
    return lax.dot_general(left, right, (((0,), (0,)), ((), ())), preferred_element_type=F32)


def shards(asked_for, offered, contents, out_weight):
    nb, nc = lax.axis_size("batch"), lax.axis_size("ctx")
    ny, nx = grid_of(nb)
    _, tokens, heads, size = asked_for.shape
    count = tokens * nc
    part, columns = out_weight.shape
    half = columns // 2
    me, at = lax.axis_index("batch"), lax.axis_index("ctx")
    my, mx = me // nx, me % nx
    cores = 2 if nc % 2 == 0 else 1
    core = at % cores
    slab = part // cores

    def piece(column):
        return lax.dynamic_slice(out_weight, (core * slab, column), (slab, half))

    swap = [(i, i ^ 1) for i in range(nc)]

    def fetched(block, perm):
        near = lax.ppermute(block, "batch", perm)
        if cores == 1:
            return (near,)
        return near, lax.ppermute(near, "ctx", swap)

    fetch_x = [fetched(piece(0), moves(ny, nx, 0, -j)) for j in range(1, nx)]
    fetch_y = [fetched(piece(half), moves(ny, nx, -j, 0)) for j in range(1, ny)]

    pairs, lanes = heads // 2, 2 * size
    paired = lambda v: v[0].transpose(1, 2, 0).reshape(pairs, lanes, tokens)
    key = to_features(paired(offered))
    value = paired(contents)
    both = jnp.einsum("pdt,pet->pde", key, value, preferred_element_type=F32)
    low = lax.broadcasted_iota(jnp.int32, (1, 1, lanes), 2) < size
    state = jnp.where(low, both[:, :size], both[:, size:])
    mass = jnp.einsum("rt,pdt->prd", jnp.ones((8, tokens), BF16), key, preferred_element_type=F32)
    packed = (jnp.concatenate([state, mass], axis=1) / count).astype(BF16)
    rows = size + 8
    packed = packed.reshape(nc, pairs // nc, rows, lanes)
    packed = lax.all_to_all(packed, "ctx", split_axis=0, concat_axis=0, tiled=True)
    total = jnp.sum(packed.astype(F32), axis=0).astype(BF16)
    total = lax.all_gather(total, "ctx", axis=0, tiled=True)
    state, mass = total[:, :size], total[:, size : size + 1]

    query = to_features(paired(asked_for))
    zero = jnp.zeros((), BF16)
    upper = lax.broadcasted_iota(jnp.int32, (1, lanes, 1), 1) < size
    same = low == upper
    wide = jnp.where(same, jnp.concatenate([state, state], axis=1), zero)
    heavy = jnp.where(same, jnp.broadcast_to(mass, (pairs, lanes, lanes)), zero)
    top = jnp.einsum("pde,pdt->pet", wide, query, preferred_element_type=F32)
    bottom = jnp.einsum("ped,pdt->pet", heavy, query, preferred_element_type=F32)
    mixed = (top / (bottom + 0.001) * count**0.5).astype(BF16)
    mixed = mixed.reshape(ny, nx, part, tokens)

    def of_y(y):
        return lax.dynamic_index_in_dim(mixed, y, 0, keepdims=False)

    def of_x(x):
        return lax.dynamic_index_in_dim(mixed, x, 1, keepdims=False)

    def partial(chosen, mine, size_of, weight, fetches):
        pick = lambda i: lax.dynamic_index_in_dim(chosen, i % size_of, 0, keepdims=False)
        out = rows_times(pick(mine), weight)
        for j, pieces in enumerate(fetches, 1):
            block = pick(mine + j)
            for k, got in enumerate(pieces):
                which = core if k == 0 else 1 - core
                out = out + rows_times(lax.dynamic_slice_in_dim(block, which * slab, slab, 0), got)
        return out

    first, second = out_weight[:, :half], out_weight[:, half:]
    came_y = [lax.ppermute(of_y((my + j) % ny), "batch", moves(ny, nx, j, 0)) for j in range(1, ny)]
    came_x = [lax.ppermute(of_x((mx + j) % nx), "batch", moves(ny, nx, 0, j)) for j in range(1, nx)]
    back_y = [
        lax.ppermute(partial(c, mx, nx, first, fetch_x).astype(BF16), "batch", moves(ny, nx, -j, 0))
        for j, c in enumerate(came_y, 1)
    ]
    back_x = [
        lax.ppermute(partial(c, my, ny, second, fetch_y).astype(BF16), "batch", moves(ny, nx, 0, -j))
        for j, c in enumerate(came_x, 1)
    ]
    left = partial(of_y(my), mx, nx, first, fetch_x)
    for got in back_y:
        left = left + got.astype(F32)
    right = partial(of_x(mx), my, ny, second, fetch_y)
    for got in back_x:
        right = right + got.astype(F32)
    return jnp.concatenate([left, right], axis=1).astype(BF16)[None]


def solution(mesh):
    in_specs = (
        P("batch", "ctx", None, None),
        P("batch", "ctx", None, None),
        P("batch", "ctx", None, None),
        P("batch", None),
    )
    out_specs = P("batch", "ctx", None)

    return jax.shard_map(shards, mesh=mesh, in_specs=in_specs, out_specs=out_specs, check_vma=False)
```
